256 devices in a mesh: row: 16 (over y_hi, z), col: 16 (over x, y_lo, core).
Axes of the slice: x: 4, y: 4 (y_hi: 2, y_lo: 2; y = y_hi * 2 + y_lo), z: 8, core: 2. Of those that a mesh axis runs over, the one named last changes fastest.
Arguments:
- fields: float32 [1, 4, 256, 256, 256], P(None, None, 'row', 'col'), may hold values from -6 to 6
- cotangent: float32 [1, 4, 256, 256, 256], P(None, None, 'row', 'col'), may hold values from -6 to 6
- spec_weights: float32 [2, 4, 4, 16, 16, 16], replicated, may hold values from -96 to 96
- point_weights: float32 [4, 4], replicated, may hold values from -3 to 3
- bias: float32 [4], replicated, may hold values from -3 to 3
Outputs:
- grad_fields: float32 [1, 4, 256, 256, 256], P(None, None, 'row', 'col')
- grad_spectral: float32 [2, 4, 4, 16, 16, 16], replicated
The draws below stay inside these ranges and needn't reach their ends.
All inputs are finite; a program needn't handle non-finite values.
Results may differ from the reference program's by a relative error of at most 0.00011.
Values sent between devices are 32-bit elements; how exact they have to be, the bound alone decides.
A program may use at most 64 MiB of HBM per device.

```python
import jax
import jax.numpy as jnp
from jax import lax

B = 1
C = 4
NX = 256
NY = 256
NZ = 256
MX = 16
MY = 16
MZ = 16


def block_levels(rng, shape, shards, smallest, top_value):
    factor_of, own = 1.0, jax.random.fold_in(rng, 6)
    for axis_at, parts in shards:
        draws = jnp.exp(jax.random.uniform(jax.random.fold_in(own, axis_at), (parts,), jnp.float32, smallest / len(shards), top_value / len(shards)))
        factor_of = factor_of * jnp.repeat(draws, shape[axis_at] // parts).reshape([-1 if axis == axis_at else 1 for axis in range(len(shape))])
    return factor_of


def gaussian(rng, extent, scale, most, cuts=(), kind=jnp.bfloat16):
    loudness = block_levels(rng, extent, cuts, -0.22, 0.18) if cuts else 1.0
    entries = jax.random.normal(rng, extent, jnp.float32) * scale * loudness
    return jnp.minimum(jnp.maximum(entries, -most), most).astype(kind)


def setup_inputs(seed: int = 0) -> dict:
    splits = jax.random.split(jax.random.key(seed), 6)
    return {
        "fields": gaussian(splits[0], (B, C, NY, NZ, NX), 1.0, 6.0, ((2, 16), (3, 16)), jnp.float32),
        "cotangent": gaussian(splits[1], (B, C, NY, NZ, NX), 1.0, 6.0, ((2, 16), (3, 16)), jnp.float32),
        "spec_weights": gaussian(splits[2], (2, C, C, MX, MY, MZ), ((NX * NY * NZ / (4.0 * C * MX * MY * MZ)) ** 0.5), 96.0, (), jnp.float32),
        "point_weights": gaussian(splits[3], (C, C), C ** -0.5, 3.0, (), jnp.float32),
        "bias": gaussian(splits[4], (C,), 0.5, 3.0, (), jnp.float32),
    }


def crop(spectrum):
    spectrum = spectrum[..., :MX]
    spectrum = jnp.concatenate([spectrum[..., :MY // 2, :, :], spectrum[..., NY - MY // 2:, :, :]], axis=-3)
    spectrum = jnp.concatenate([spectrum[..., :MZ // 2, :], spectrum[..., NZ - MZ // 2:, :]], axis=-2)
    return spectrum

def expand(modes):
    lead = modes.shape[:2]
    modes = jnp.pad(modes, [(0, 0), (0, 0), (0, 0), (0, 0), (0, NX // 2 + 1 - MX)])
    width_x = modes.shape[4]
    zeros_z = jnp.zeros(lead + (MY, NZ - MZ, width_x), modes.dtype)
    modes = jnp.concatenate([modes[..., :MZ // 2, :], zeros_z, modes[..., MZ // 2:, :]], axis=-2)
    zeros_y = jnp.zeros(lead + (NY - MY, NZ, width_x), modes.dtype)
    modes = jnp.concatenate([modes[..., :MY // 2, :, :], zeros_y, modes[..., MY // 2:, :, :]], axis=-3)
    return modes

def spectral(fields, spec_weights):
    spectrum = crop(jnp.fft.rfftn(fields, axes=(2, 3, 4)))
    weights = spec_weights[0] + 1j * spec_weights[1]
    mixed_modes = jnp.einsum('biqrp,iopqr->boqrp', spectrum, weights, precision=lax.Precision.HIGHEST)
    return jnp.fft.irfftn(expand(mixed_modes), s=(NY, NZ, NX), axes=(2, 3, 4))

def reference(fields, cotangent, spec_weights, point_weights, bias):

    def forward(field_in, weight_in):
        local_term = jnp.einsum('bcyzx,co->boyzx', field_in, point_weights, precision=lax.Precision.HIGHEST)
        pre_activation = spectral(field_in, weight_in) + local_term + bias[None, :, None, None, None]
        return jax.nn.gelu(pre_activation, approximate=False)
    output, pullback = jax.vjp(forward, fields, spec_weights)
    grad_fields, grad_spectral = pullback(cotangent.astype(output.dtype))
    return (grad_fields, grad_spectral)
```

```python
import functools
import math

import jax
import jax.numpy as jnp
import numpy as np
from jax import lax
from jax.experimental import pallas as pl
from jax.experimental.pallas import tpu as pltpu
from jax.sharding import PartitionSpec as P

C = 4
N = 256
MODES = 16
CELLS = 256
LINES = 16
PLANE = 32
DEPTH = 8
MESH = pl.DeviceIdType.MESH
f32 = jnp.float32
bf16 = jnp.bfloat16
NT = (((1,), (1,)), ((), ()))


def signed_table(outer):
    wave = np.where(np.arange(MODES) < MODES // 2, np.arange(MODES), np.arange(MODES) - MODES)
    points = np.arange(N)
    angle = 2.0 * np.pi / N * (points[:, None] * wave[None, :] % N)
    angle = np.repeat(angle, MODES, 1) if outer else np.tile(angle, (1, MODES))
    return np.concatenate([np.cos(angle), np.sin(angle)], 1).astype(np.float32)


def split_constant(table):
    high = table.astype(jnp.bfloat16)
    low = (table - high.astype(np.float64)).astype(jnp.bfloat16)
    return high, low


def x_angles():
    return 2.0 * np.pi / N * (np.arange(MODES)[:, None] * np.arange(N)[None, :] % N)


def analysis_constant():
    angle = x_angles()
    high, low = split_constant(np.concatenate([np.cos(angle), -np.sin(angle)], 0))
    return np.concatenate([high, low], 0)


def synthesis_constant():
    angle = x_angles()
    weight = np.where(np.arange(MODES) == 0, 1.0, 2.0)[:, None] / float(N) ** 3
    high, low = split_constant(np.concatenate([np.cos(angle) * weight, -np.sin(angle) * weight], 0))
    full = np.zeros((C, 384, N), high.dtype)
    for c in range(C):
        full[c, c * 32 : c * 32 + 32] = high
        full[c, 128 + c * 32 : 128 + c * 32 + 32] = high
        full[c, 256 + c * 32 : 256 + c * 32 + 32] = low
    return full


def halves(value):
    high = value.astype(bf16)
    low = (value - high.astype(f32)).astype(bf16)
    return high, low


def dot(a, b):
    return jnp.dot(a, b, preferred_element_type=f32)


def dot_nt(a, b):
    return lax.dot_general(a, b, NT, preferred_element_type=f32)


def analyse_x(tx, block):
    high, low = halves(block)
    both = dot_nt(tx[...], high)
    return both[:32] + both[32:] + dot_nt(tx[0:32, :], low)


def analyse_yz(lines, eh, el, tiles):
    high, low = halves(lines[...])
    both = dot(jnp.concatenate([high, low], 0), eh[...])
    part = both[:128] + both[128:] + dot(high, el[...])
    for c in range(C):
        re = part[c * 32 : c * 32 + 16]
        im = part[c * 32 + 16 : c * 32 + 32]
        pair = (re[:, :256] + im[:, 256:], im[:, :256] - re[:, 256:])
        for t in range(2):
            for half in range(2):
                for side in range(2):
                    tiles[t * 16 + (c * 2 + half) * 2 + side] = pair[t][
                        half * 8 : half * 8 + 8, side * 128 : side * 128 + 128
                    ]


def spectrum_of(tiles, t, c):
    rows = []
    for half in range(2):
        k = t * 16 + (c * 2 + half) * 2
        rows.append(jnp.concatenate([tiles[k], tiles[k + 1]], 1))
    return jnp.concatenate(rows, 0)


def synth_yz(modes, eh, el):
    rows = []
    for re, im in modes:
        rows.append(jnp.concatenate([re, -im], 1))
        rows.append(jnp.concatenate([im, re], 1))
    high, low = halves(jnp.concatenate(rows, 0))
    both = dot_nt(eh[...], jnp.concatenate([high, low], 0))
    lines = both[:, :128] + both[:, 128:] + dot_nt(el[...], high)
    high, low = halves(lines)
    return jnp.concatenate([high, low, high], 1)


def device_of(z, rank):
    return {"row": rank // 16 * DEPTH + z, "col": lax.rem(rank, 16)}


def comm_kernel(
    fields,
    cot,
    weights,
    ty,
    tz,
    tx_in,
    ts_in,
    point,
    bias,
    local_out,
    su_out,
    sh_out,
    wm_out,
    eh_out,
    el_out,
    fv,
    cv,
    lv,
    wv,
    tyv,
    tzv,
    tx,
    ts,
    lines,
    part_u,
    part_h,
    rs_u,
    rs_h,
    zs_u,
    zs_h,
    zr_u,
    zr_h,
    ag_u,
    ag_h,
    load_sem,
    send_sem,
    recv_sem,
):
    row = lax.axis_index("row")
    col = lax.axis_index("col")
    z = lax.rem(row, DEPTH)
    me = row // DEPTH * 16 + col

    loads = [
        pltpu.make_async_copy(ty.at[pl.ds(pl.multiple_of(row * LINES, 8), LINES)], tyv, load_sem.at[0]),
        pltpu.make_async_copy(tz.at[pl.ds(pl.multiple_of(col * LINES, 8), LINES)], tzv, load_sem.at[1]),
        pltpu.make_async_copy(tx_in, tx, load_sem.at[2]),
    ]
    for c in range(C):
        spot = pl.ds(c * CELLS, CELLS)
        loads.append(pltpu.make_async_copy(fields.at[spot], fv.at[spot], load_sem.at[3 + c]))
    loads.append(pltpu.make_async_copy(weights, wv, load_sem.at[7]))
    loads.append(pltpu.make_async_copy(ts_in, ts, load_sem.at[8]))
    loads.append(pltpu.make_async_copy(cot, cv, load_sem.at[9]))
    for load in loads:
        load.start()

    barrier = pltpu.get_barrier_semaphore()

    def greet_plane(step, carry):
        peer = lax.rem(me + step, PLANE)
        pl.semaphore_signal(barrier, inc=1, device_id=device_of(z, peer), device_id_type=MESH)
        return carry

    lax.fori_loop(1, PLANE, greet_plane, 0)

    def greet_depth(step, carry):
        peer = lax.rem(z + step, DEPTH)
        pl.semaphore_signal(barrier, inc=1, device_id=device_of(peer, me), device_id_type=MESH)
        return carry

    lax.fori_loop(1, DEPTH, greet_depth, 0)

    for k in range(3):
        loads[k].wait()
    cz = tzv[:, :256]
    sz = tzv[:, 256:]
    for y in range(LINES):
        cy = tyv[y : y + 1, :256]
        sy = tyv[y : y + 1, 256:]
        high, low = halves(jnp.concatenate([cy * cz - sy * sz, sy * cz + cy * sz], 1))
        eh_out[y * LINES : (y + 1) * LINES, :] = high
        el_out[y * LINES : (y + 1) * LINES, :] = low

    for c in range(C):
        loads[3 + c].wait()
        lines[c * 32 : c * 32 + 32, :] = analyse_x(tx, fv[c * CELLS : (c + 1) * CELLS, :])
    analyse_yz(lines, eh_out, el_out, part_u)

    pl.semaphore_wait(barrier, PLANE - 1 + DEPTH - 1)

    def copy_to(src, dst, sem, device):
        return pltpu.make_async_remote_copy(
            src_ref=src,
            dst_ref=dst,
            send_sem=send_sem.at[sem],
            recv_sem=recv_sem.at[sem],
            device_id=device,
            device_id_type=MESH,
        )

    def start_scatter(part, rs, sem):
        def send(step, carry):
            peer = lax.rem(me + step, PLANE)
            copy_to(part.at[peer], rs.at[me], sem, device_of(z, peer)).start()
            return carry

        lax.fori_loop(1, PLANE, send, 0)
        rs[me] = part[me]

    def finish_scatter(part, rs, sem):
        both = copy_to(
            part.at[pl.ds(0, PLANE - 1)], rs.at[pl.ds(0, PLANE - 1)], sem, device_of(z, me)
        )
        both.wait_recv()
        return both

    def exchange_depth(total, zs, zr, sem):
        zs[0] = total
        zr[z] = total

        def send(step, carry):
            peer = lax.rem(z + step, DEPTH)
            copy_to(zs.at[0], zr.at[z], sem, device_of(peer, me)).start()
            return carry

        lax.fori_loop(1, DEPTH, send, 0)
        both = copy_to(
            zr.at[pl.ds(0, DEPTH - 1)], zr.at[pl.ds(0, DEPTH - 1)], sem, device_of(z, me)
        )
        both.wait_recv()
        return both

    def gather_plane(total, zs, ag, sem):
        zs[1] = total
        ag[me] = total

        def send(step, carry):
            peer = lax.rem(me + step, PLANE)
            copy_to(zs.at[1], ag.at[me], sem, device_of(z, peer)).start()
            return carry

        lax.fori_loop(1, PLANE, send, 0)
        both = copy_to(
            ag.at[pl.ds(0, PLANE - 1)], ag.at[pl.ds(0, PLANE - 1)], sem, device_of(z, me)
        )
        both.wait_recv()
        return both

    def sum_tiles(ref, count):
        values = [ref[k] for k in range(count)]
        while len(values) > 1:
            values = [values[k] + values[k + 1] for k in range(0, len(values), 2)]
        return values[0]

    def finish_reduce(part, rs, zs, zr, ag, sem):
        done = [finish_scatter(part, rs, sem)]
        done.append(exchange_depth(sum_tiles(rs, PLANE), zs, zr, sem + 1))
        done.append(gather_plane(sum_tiles(zr, DEPTH), zs, ag, sem + 2))
        return done

    start_scatter(part_u, rs_u, 0)

    def local_terms(block, carry):
        at = block * 32
        inputs = [fv[pl.ds(pl.multiple_of(i * CELLS + at, 8), 32), :] for i in range(C)]
        for o in range(C):
            value = inputs[0] * point[0, o] + bias[o]
            for i in range(1, C):
                value = value + inputs[i] * point[i, o]
            lv[pl.ds(pl.multiple_of(o * CELLS + at, 8), 32), :] = value
        return carry

    lax.fori_loop(0, CELLS // 32, local_terms, 0)
    loads[7].wait()
    for q in range(MODES):
        wm_out[:, q * 16 : q * 16 + 16] = wv[pl.ds(q, 512, stride=MODES), :]
    loads[8].wait()
    loads[9].wait()

    done = finish_reduce(part_u, rs_u, zs_u, zr_u, ag_u, 0)

    def weight(t, i, o):
        at = ((t * C + i) * C + o) * MODES
        return wm_out[at : at + MODES, :]

    modes = []
    for o in range(C):
        re = im = 0.0
        for i in range(C):
            ur, ui = spectrum_of(ag_u, 0, i), spectrum_of(ag_u, 1, i)
            wr, wi = weight(0, i, o), weight(1, i, o)
            re = re + (ur * wr - ui * wi)
            im = im + (ur * wi + ui * wr)
        modes.append((re, im))
    synth = synth_yz(modes, eh_out, el_out)

    for c in range(C):
        base = c * CELLS
        lv[base : base + CELLS, :] += dot(synth, ts[c])

        def slope(block, carry):
            at = pl.ds(pl.multiple_of(base + block * 32, 8), 32)
            v = lv[at, :]
            cdf = 0.5 * (1.0 + lax.erf(v * (1.0 / math.sqrt(2.0))))
            density = jnp.exp(-0.5 * v * v) * (1.0 / math.sqrt(2.0 * math.pi))
            cv[at, :] = cv[at, :] * (cdf + v * density)
            return carry

        lax.fori_loop(0, CELLS // 32, slope, 0)
        lines[c * 32 : c * 32 + 32, :] = analyse_x(tx, cv[base : base + CELLS, :])
    analyse_yz(lines, eh_out, el_out, part_h)

    start_scatter(part_h, rs_h, 3)

    def back_terms(block, carry):
        at = block * 32
        outputs = [cv[pl.ds(pl.multiple_of(o * CELLS + at, 8), 32), :] for o in range(C)]
        for i in range(C):
            value = outputs[0] * point[i, 0]
            for o in range(1, C):
                value = value + outputs[o] * point[i, o]
            local_out[pl.ds(pl.multiple_of(i * CELLS + at, 8), 32), :] = value
        return carry

    lax.fori_loop(0, CELLS // 32, back_terms, 0)
    for k in range(PLANE):
        su_out[k] = ag_u[k]

    done += finish_reduce(part_h, rs_h, zs_h, zr_h, ag_h, 3)
    for k in range(PLANE):
        sh_out[k] = ag_h[k]
    for both in done:
        both.wait_send()


def final_kernel(local, su, sh, wm, eh, el, ts, grad_fields, grad_weights):
    def weight(t, i, o):
        at = ((t * C + i) * C + o) * MODES
        return wm[at : at + MODES, :]

    modes = []
    for i in range(C):
        re = im = 0.0
        for o in range(C):
            hr, hi = spectrum_of(sh, 0, o), spectrum_of(sh, 1, o)
            wr, wi = weight(0, i, o), weight(1, i, o)
            re = re + (wr * hr + wi * hi)
            im = im + (wr * hi - wi * hr)
        modes.append((re, im))
    synth = synth_yz(modes, eh, el)
    for c in range(C):
        at = slice(c * CELLS, (c + 1) * CELLS)
        grad_fields[at, :] = local[at, :] + dot(synth, ts[c])

    wave = lax.broadcasted_iota(jnp.int32, (MODES, 256), 0)
    factor = jnp.where(wave == 0, 1.0, 2.0).astype(f32) * (1.0 / float(N) ** 3)
    for i in range(C):
        ur, ui = spectrum_of(su, 0, i) * factor, spectrum_of(su, 1, i) * factor
        for o in range(C):
            hr, hi = spectrum_of(sh, 0, o), spectrum_of(sh, 1, o)
            pair = (ur * hr + ui * hi, ur * hi - ui * hr)
            for t in range(2):
                at = ((t * C + i) * C + o) * MODES * MODES
                for q in range(MODES):
                    grad_weights[pl.ds(at + q, MODES, stride=MODES), :] = pair[t][
                        :, q * 16 : q * 16 + 16
                    ]


def per_device(fields, cotangent, spec_weights, point_weights, bias):
    vmem = pl.BlockSpec(memory_space=pltpu.VMEM)
    smem = pl.BlockSpec(memory_space=pltpu.SMEM)
    anywhere = pl.BlockSpec(memory_space=pl.ANY)
    tile = (8, 128)
    ts = jnp.asarray(synthesis_constant())
    local, su, sh, wm, eh, el = pl.pallas_call(
        comm_kernel,
        out_shape=(
            jax.ShapeDtypeStruct((C * CELLS, N), f32),
            jax.ShapeDtypeStruct((PLANE, *tile), f32),
            jax.ShapeDtypeStruct((PLANE, *tile), f32),
            jax.ShapeDtypeStruct((512, 256), f32),
            jax.ShapeDtypeStruct((256, 512), bf16),
            jax.ShapeDtypeStruct((256, 512), bf16),
        ),
        in_specs=[anywhere] * 7 + [smem] * 2,
        out_specs=[vmem] * 6,
        scratch_shapes=[
            pltpu.VMEM((C * CELLS, N), f32),
            pltpu.VMEM((C * CELLS, N), f32),
            pltpu.VMEM((C * CELLS, N), f32),
            pltpu.VMEM((8192, 16), f32),
            pltpu.VMEM((LINES, 512), f32),
            pltpu.VMEM((LINES, 512), f32),
            pltpu.VMEM((64, N), bf16),
            pltpu.VMEM((C, 384, N), bf16),
            pltpu.VMEM((128, 256), f32),
            pltpu.VMEM((PLANE, *tile), f32),
            pltpu.VMEM((PLANE, *tile), f32),
            pltpu.VMEM((PLANE, *tile), f32),
            pltpu.VMEM((PLANE, *tile), f32),
            pltpu.VMEM((2, *tile), f32),
            pltpu.VMEM((2, *tile), f32),
            pltpu.VMEM((DEPTH, *tile), f32),
            pltpu.VMEM((DEPTH, *tile), f32),
            pltpu.VMEM((PLANE, *tile), f32),
            pltpu.VMEM((PLANE, *tile), f32),
            pltpu.SemaphoreType.DMA((10,)),
            pltpu.SemaphoreType.DMA((6,)),
            pltpu.SemaphoreType.DMA((6,)),
        ],
        compiler_params=pltpu.CompilerParams(collective_id=0, has_side_effects=True),
        name="spectra",
    )(
        fields.reshape(C * CELLS, N),
        cotangent.reshape(C * CELLS, N),
        spec_weights.reshape(8192, 16),
        jnp.asarray(signed_table(True)),
        jnp.asarray(signed_table(False)),
        jnp.asarray(analysis_constant()),
        ts,
        point_weights,
        bias,
    )
    grad_fields, grad_weights = pl.pallas_call(
        final_kernel,
        out_shape=(
            jax.ShapeDtypeStruct((C * CELLS, N), f32),
            jax.ShapeDtypeStruct((8192, 16), f32),
        ),
        in_specs=[vmem] * 7,
        out_specs=[vmem] * 2,
        name="gradients",
    )(local, su, sh, wm, eh, el, ts)
    return (
        grad_fields.reshape(1, C, LINES, LINES, N),
        grad_weights.reshape(2, C, C, MODES, MODES, MODES),
    )


def solution(mesh):
    placed = (P(None, None, "row", "col", None), P(None, None, "row", "col", None), P(), P(), P())
    return jax.shard_map(
        per_device,
        mesh=mesh,
        in_specs=placed,
        out_specs=(P(None, None, "row", "col", None), P()),
        check_vma=False,
    )
```
